32 devices in a mesh: gx: 4 (over x, core), gy: 2 (over y), gz: 4 (over z).
Axes of the slice: x: 2, y: 2, z: 4, core: 2. Of those that a mesh axis runs over, the one named last changes fastest.
Arguments:
- warped_image: float32 [256, 128, 512], P('gx', 'gy', 'gz'), may hold values from -6 to 6
- fixed_image: float32 [256, 128, 512], P('gx', 'gy', 'gz'), may hold values from -6 to 6
- fine_control: float32 [3, 32, 16, 64], P(None, 'gx', 'gy', 'gz'), may hold values from -6 to 6
- coarse_control: float32 [3, 8, 4, 16], replicated, may hold values from -6 to 6
Outputs:
- fine_gradient: float32 [3, 32, 16, 64], P(None, 'gx', 'gy', 'gz')
- coarse_gradient: float32 [3, 8, 4, 16], replicated
The draws below stay inside these ranges and needn't reach their ends.
All inputs are finite; a program needn't handle non-finite values.
Results may differ from the reference program's by a relative error of at most 0.0003.
Values sent between devices are 32-bit elements; how exact they have to be, the bound alone decides.
A program may use at most 64 MiB of HBM per device.

```python
import jax
import jax.numpy as jnp
from jax import lax

SPF = 8
SPC = 32
NX = 256
NY = 128
NZ = 512
FX = 32
FY = 16
FZ = 64
KX = 8
KY = 4
KZ = 16


def levels(key, shape, shards, low, largest):
    def one(position, shards_of):
        draws = jax.random.uniform(jax.random.fold_in(jax.random.fold_in(key, 6), position), (shards_of,), jnp.float32, low / len(shards), largest / len(shards))
        return jnp.repeat(jnp.exp(draws), shape[position] // shards_of).reshape((-1,) + (1,) * (len(shape) - position - 1))

    gain = one(*shards[0])
    for cut in shards[1:]:
        gain = gain * one(*cut)
    return gain


def scatter_about(rng, extent, deviation, most, cuts=(), kind=jnp.bfloat16):
    entries = deviation * jax.random.normal(rng, extent, jnp.float32)
    if cuts:
        entries = entries * levels(rng, extent, cuts, -0.22, 0.18)
    return jnp.clip(entries, -most, most).astype(kind)


def setup_inputs(seed: int = 0) -> dict:
    arg_keys = jax.random.split(jax.random.key(seed), 5)
    return {
        "warped_image": scatter_about(arg_keys[0], (NX, NY, NZ), 1.0, 6.0, ((0, 4), (1, 2), (2, 4)), jnp.float32),
        "fixed_image": scatter_about(arg_keys[1], (NX, NY, NZ), 1.0, 6.0, ((0, 4), (1, 2), (2, 4)), jnp.float32),
        "fine_control": scatter_about(arg_keys[2], (3, FX, FY, FZ), 1.0, 6.0, ((1, 4), (2, 2), (3, 4)), jnp.float32),
        "coarse_control": scatter_about(arg_keys[3], (3, KX, KY, KZ), 1.0, 6.0, (), jnp.float32),
    }


bend_factor = 0.01
highest = lax.Precision.HIGHEST


def spline(values):
    magnitude = jnp.abs(values)
    inner = 2.0 / 3.0 - magnitude * magnitude + 0.5 * magnitude * magnitude * magnitude
    remain = 2.0 - magnitude
    outer = remain * remain * remain / 6.0
    return jnp.where(magnitude < 1.0, inner, jnp.where(magnitude < 2.0, outer, 0.0 * magnitude))


def basis_matrix(voxels, points, spacing, voxel_start, point_start):
    voxel = (jnp.arange(voxels, dtype=jnp.int32) + voxel_start).astype(jnp.float32) + 0.5
    centre = (jnp.arange(points, dtype=jnp.int32) + point_start).astype(jnp.float32) * spacing + 0.5 * spacing
    return spline((voxel[:, None] - centre[None, :]) / spacing)


def slope(padded, axis):
    rank = padded.ndim
    count = padded.shape[axis] - 4

    def shifted(offset):
        piece = lax.slice_in_dim(padded, offset, offset + count, axis=axis)
        for other in range(rank - 3, rank):
            if other != axis:
                piece = lax.slice_in_dim(piece, 2, piece.shape[other] - 2, axis=other)
        return piece

    return (shifted(0) - 8.0 * shifted(1) + 8.0 * shifted(3) - shifted(4)) / 12.0


def stencil(padded):
    centre = padded[:, 1:-1, 1:-1, 1:-1]
    total = padded[:, 2:, 1:-1, 1:-1] + padded[:, :-2, 1:-1, 1:-1]
    total = total + padded[:, 1:-1, 2:, 1:-1] + padded[:, 1:-1, :-2, 1:-1]
    total = total + padded[:, 1:-1, 1:-1, 2:] + padded[:, 1:-1, 1:-1, :-2]
    return total - 6.0 * centre


def laplace(field):
    return stencil(jnp.pad(field, ((0, 0), (1, 1), (1, 1), (1, 1))))


def project_blocks(force, along_x, along_y, along_z):
    section = jnp.einsum("axyz,zr->axyr", force, along_z, precision=highest)
    section = jnp.einsum("axyr,yq->axqr", section, along_y, precision=highest)
    return jnp.einsum("axqr,xp->apqr", section, along_x, precision=highest)


def reference(warped_image, fixed_image, fine_control, coarse_control):
    summed = jnp.pad(warped_image + fixed_image, 2)
    difference = warped_image - fixed_image
    fine_x = basis_matrix(NX, FX, SPF, 0, 0)
    fine_y = basis_matrix(NY, FY, SPF, 0, 0)
    fine_z = basis_matrix(NZ, FZ, SPF, 0, 0)
    coarse_x = basis_matrix(NX, KX, SPC, 0, 0)
    coarse_y = basis_matrix(NY, KY, SPC, 0, 0)
    coarse_z = basis_matrix(NZ, KZ, SPC, 0, 0)
    block_rows = 16

    def block(carry, start):
        fine_sum, coarse_sum = carry
        slab = lax.dynamic_slice_in_dim(summed, start, block_rows + 4, 0)
        slopes = jnp.stack([slope(slab, 0), slope(slab, 1), slope(slab, 2)]) * 0.5
        local = lax.dynamic_slice_in_dim(difference, start, block_rows, 0)
        force = slopes * local[None]
        fine_rows = lax.dynamic_slice_in_dim(fine_x, start, block_rows, 0)
        coarse_rows = lax.dynamic_slice_in_dim(coarse_x, start, block_rows, 0)
        fine_sum = fine_sum + project_blocks(force, fine_rows, fine_y, fine_z)
        coarse_sum = coarse_sum + project_blocks(force, coarse_rows, coarse_y, coarse_z)
        return (fine_sum, coarse_sum), None

    starts = jnp.arange(NX // block_rows, dtype=jnp.int32) * block_rows
    initial = (jnp.zeros((3, FX, FY, FZ), jnp.float32), jnp.zeros((3, KX, KY, KZ), jnp.float32))
    (fine_sum, coarse_sum), _ = lax.scan(block, initial, starts)
    fine_gradient = fine_sum * (SPF ** -1.5) + bend_factor * laplace(laplace(fine_control))
    coarse_gradient = coarse_sum * (SPC ** -1.5) + bend_factor * laplace(laplace(coarse_control))
    return fine_gradient, coarse_gradient
```

```python
import functools

import jax
import jax.numpy as jnp
from jax import lax
from jax.experimental import pallas as pl
from jax.experimental.pallas import tpu as pltpu
from jax.sharding import PartitionSpec as P

SPF = 8
SPC = 32
BEND = 0.01
HI = lax.Precision.HIGHEST
MESH = pl.DeviceIdType.MESH
f32 = jnp.float32
bf16 = jnp.bfloat16


def nn(a, b):
    return lax.dot_general(
        a, b, (((1,), (0,)), ((), ())), precision=HI, preferred_element_type=f32
    )


def nt(a, b):
    return lax.dot_general(
        a, b, (((1,), (1,)), ((), ())), precision=HI, preferred_element_type=f32
    )


def spline(t):
    m = jnp.abs(t)
    inner = 2.0 / 3.0 - m * m + 0.5 * m * m * m
    r = 2.0 - m
    outer = r * r * r * (1.0 / 6.0)
    return jnp.where(m < 1.0, inner, jnp.where(m < 2.0, outer, 0.0))


def weight(voxel, point, spacing):
    scaled = (2 * voxel + 1 - spacing * (2 * point + 1)).astype(f32)
    return spline(scaled * (0.5 / spacing))


def iota(shape, axis):
    return lax.broadcasted_iota(jnp.int32, shape, axis)


def diff1(out, inp):
    d = jnp.abs(out - inp)
    return jnp.where(d == 0, -2.0, jnp.where(d == 1, 1.0, 0.0)).astype(f32)


def diff2(out, inp, count):
    d = jnp.abs(out - inp)
    edge = (inp == 0) | (inp == count - 1)
    centre = jnp.where(edge, 5.0, 6.0)
    return jnp.where(
        d == 0, centre, jnp.where(d == 1, -4.0, jnp.where(d == 2, 1.0, 0.0))
    ).astype(f32)


def same(out, inp):
    return jnp.where(out == inp, 1.0, 0.0).astype(f32)


def bend_planes(px, py, qx, qy, cx, cy):
    jx, jy = same(px, qx), same(py, qy)
    tx, ty = diff1(px, qx), diff1(py, qy)
    m0 = diff2(px, qx, cx) * jy + jx * diff2(py, qy, cy) + 2.0 * tx * ty
    m1 = 2.0 * (tx * jy + jx * ty)
    return m0 * BEND, m1 * BEND, jx * jy * BEND


def kernel(sizes, w_hbm, f_hbm, fc_ref, cc_ref, fo_ref, co_ref,
           w_v, f_v, s_v, ysend, yrecv, zsend, zrecv, zcorr, wf_v, wc_v, fh_v, fl_v,
           accf, accc, tz_v, bend_v, ccp, bendc, zmsg, zgot, a_v, agot, b_v, bgot,
           cslots, load_sem, hs_sem, hr_sem, ms_sem, mr_sem, cs_sem, cr_sem):
    nx, ny, nz = sizes
    axes = ("gx", "gy", "gz")
    counts = sizes
    me = [lax.axis_index(a) for a in axes]
    SX, SY, SZ = w_v.shape
    PX, PY, PZ = SX // SPF, SY // SPF, SZ // SPF
    EX, QE, QC = PX + 4, 16, accc.shape[1]
    KX, KY, KZ = cc_ref.shape[1:]
    cells = SX // SPF
    lanes = 3 * SZ

    loads = []
    for c in range(cells):
        part = pl.ds(c * SPF, SPF)
        loads.append((
            pltpu.make_async_copy(w_hbm.at[part], w_v.at[part], load_sem.at[0, c]),
            pltpu.make_async_copy(f_hbm.at[part], f_v.at[part], load_sem.at[1, c]),
        ))
    for one, two in loads:
        one.start()
        two.start()

    zero_plane = jnp.zeros((2, SY, SZ), f32)
    s_v[0:2, 8:8 + SY, :] = zero_plane
    s_v[SX + 2:SX + 4, 8:8 + SY, :] = zero_plane
    yrecv[...] = jnp.zeros(yrecv.shape, f32)
    zrecv[...] = jnp.zeros(zrecv.shape, f32)
    zgot[...] = jnp.zeros(zgot.shape, f32)
    agot[...] = jnp.zeros(agot.shape, f32)
    bgot[...] = jnp.zeros(bgot.shape, f32)

    barrier = pltpu.get_barrier_semaphore()
    total = 0
    for k, a in enumerate(axes):
        for d in range(1, counts[k]):
            pl.semaphore_signal(
                barrier, inc=1, device_id={a: lax.rem(me[k] + d, counts[k])}, device_id_type=MESH
            )
            total += 1

    def split_store(ref, index, value):
        high = value.astype(bf16)
        ref[index + (0,)] = high
        ref[index + (1,)] = (value - high.astype(f32)).astype(bf16)

    KC = SPF * SY
    rows, cols = iota((5 * QE, KC), 0), iota((5 * QE, KC), 1)
    split_store(wf_v, (), weight(cols // SY, rows // QE - 2, SPF)
                * weight(cols % SY, rows % QE - 2, SPF))
    rows, cols = iota((4 * QC, KC), 0), iota((4 * QC, KC), 1)
    along_y = weight(cols % SY + me[1] * SY, rows % QC, SPC)
    for ph in range(SPC // SPF):
        first = -2 if ph < SPC // SPF // 2 else -1
        split_store(wc_v, (ph,),
                    weight(cols // SY + ph * SPF, rows // QC + first, SPC) * along_y)

    lane = iota((SY, SZ), 1)

    def one_slab(x, carry):
        low, high = carry
        s = w_v[x] + f_v[x]
        s_v[x + 2, 8:8 + SY, :] = s
        ysend[0, x] = s[0:2]
        ysend[1, x] = s[SY - 2:SY]
        here = lane // 2 == x
        low = jnp.where(here, pltpu.roll(s, 2 * x, 1), low)
        high = jnp.where(here, pltpu.roll(s, lax.rem(2 * x + 2, SZ), 1), high)
        return low, high

    carry = (jnp.zeros((SY, SZ), f32), jnp.zeros((SY, SZ), f32))
    for c in range(cells):
        for copy in loads[c]:
            copy.wait()
        carry = lax.fori_loop(c * SPF, (c + 1) * SPF, one_slab, carry)
    zsend[0] = carry[0]
    zsend[1] = carry[1]

    pl.semaphore_wait(barrier, total)

    has = [(me[k] > 0, me[k] < counts[k] - 1) for k in range(3)]

    def halo(k, side):
        if k == 0:
            src = s_v.at[pl.ds(2 if side == 0 else SX, 2), pl.ds(8, SY), :]
            dst = s_v.at[pl.ds(SX + 2 if side == 0 else 0, 2), pl.ds(8, SY), :]
        elif k == 1:
            src, dst = ysend.at[side], yrecv.at[1 - side]
        else:
            src, dst = zsend.at[side], zrecv.at[1 - side]
        return neighbour_copy(k, side, src, dst, hs_sem.at[k, side], hr_sem.at[k, 1 - side])

    def neighbour_copy(k, side, src, dst, send, recv):
        other = me[k] - 1 if side == 0 else me[k] + 1
        return pltpu.make_async_remote_copy(
            src_ref=src, dst_ref=dst, send_sem=send, recv_sem=recv,
            device_id={axes[k]: other}, device_id_type=MESH,
        )

    for k in (2, 1, 0):
        for side in range(2):
            @pl.when(has[k][side])
            def _(k=k, side=side):
                halo(k, side).start()

    accf[...] = jnp.zeros(accf.shape, f32)
    accc[...] = jnp.zeros(accc.shape, f32)
    shape = (EX * QE, PX * PY)
    rows, cols = iota(shape, 0), iota(shape, 1)
    ox, oy = me[0] * PX, me[1] * PY
    planes = bend_planes(rows // QE - 2 + ox, rows % QE - 2 + oy,
                         cols // PY + ox, cols % PY + oy, PX * nx, PY * ny)
    RZ = tz_v.shape[1]

    def ext_point(row):
        return jnp.where(row < PZ, row, jnp.where(row < PZ + 2, row - PZ - 2, row - 2))

    oz = me[2] * PZ
    zr, zc = ext_point(iota((RZ, PZ), 0)) + oz, iota((RZ, PZ), 1) + oz
    along = (same(zr, zc), diff1(zr, zc), diff2(zr, zc, PZ * nz))
    for a in range(3):
        block = fc_ref[a].reshape(PX * PY, PZ)
        bend_v[a] = (nt(along[0], nn(planes[0], block)) + nt(along[1], nn(planes[1], block))
                     + nt(along[2], nn(planes[2], block)))
    shape = (KX * QC, KX * QC)
    rows, cols = iota(shape, 0), iota(shape, 1)
    planes = bend_planes(rows // QC, rows % QC, cols // QC, cols % QC, KX, KY)
    zr, zc = iota((KZ, KZ), 0), iota((KZ, KZ), 1)
    ccp[...] = jnp.zeros(ccp.shape, f32)
    for a in range(3):
        for p in range(KX):
            ccp[a, p * QC:p * QC + KY, :] = cc_ref[a, p]
        block = ccp[a]
        bendc[a] = (nn(planes[0], block) + nn(planes[1], nn(block, diff1(zr, zc)))
                    + BEND * nn(block, diff2(zr, zc, KZ)))

    for k in (2, 1, 0):
        for side in range(2):
            @pl.when(has[k][side])
            def _(k=k, side=side):
                copy = halo(k, side)
                copy.wait_send()

            @pl.when(has[k][1 - side])
            def _(k=k, side=side):
                halo(k, side).wait_recv()

    even = lane % 2 == 0
    dl = zrecv[0] - zsend[1]
    dh = zrecv[1] - zsend[0]
    zcorr[0] = jnp.where(even, dl - 8.0 * pltpu.roll(dl, SZ - 1, 1), dl)
    zcorr[1] = jnp.where(even, -dh, 8.0 * pltpu.roll(dh, 1, 1) - dh)

    def cell(i, _):
        k = i // (SPC // SPF)
        ph = i % (SPC // SPF)
        for xx in range(SPF):
            x = i * SPF + xx
            s_v[x + 2, 6:8, :] = yrecv[0, x]
            s_v[x + 2, 8 + SY:10 + SY, :] = yrecv[1, x]
            d = w_v[x] - f_v[x]
            s = s_v[x + 2, 8:8 + SY, :]
            gx = (s_v[x, 8:8 + SY, :] - s_v[x + 4, 8:8 + SY, :]
                  + 8.0 * (s_v[x + 3, 8:8 + SY, :] - s_v[x + 1, 8:8 + SY, :]))
            gy = (s_v[x + 2, 6:6 + SY, :] - s_v[x + 2, 10:10 + SY, :]
                  + 8.0 * (s_v[x + 2, 9:9 + SY, :] - s_v[x + 2, 7:7 + SY, :]))
            gz = (pltpu.roll(s, 2, 1) - pltpu.roll(s, SZ - 2, 1)
                  + 8.0 * (pltpu.roll(s, SZ - 1, 1) - pltpu.roll(s, 1, 1)))
            corr = jnp.where(lane < 2, pltpu.roll(zcorr[0], lax.rem(SZ - 2 * x, SZ), 1), 0.0)
            corr = jnp.where(lane >= SZ - 2,
                             pltpu.roll(zcorr[1], lax.rem(2 * SZ - 2 - 2 * x, SZ), 1), corr)
            gz = gz + corr
            for a, g in enumerate((gx, gy, gz)):
                force = g * d
                high = force.astype(bf16)
                fh_v[xx * SY:(xx + 1) * SY, a * SZ:(a + 1) * SZ] = high
                fl_v[xx * SY:(xx + 1) * SY, a * SZ:(a + 1) * SZ] = (
                    force - high.astype(f32)).astype(bf16)
        wh = jnp.concatenate([wf_v[0], wc_v[ph, 0]], axis=0)
        wl = jnp.concatenate([wf_v[1], wc_v[ph, 1]], axis=0)
        out = (jnp.dot(wh, fh_v[...], preferred_element_type=f32)
               + jnp.dot(wl, fh_v[...], preferred_element_type=f32)
               + jnp.dot(wh, fl_v[...], preferred_element_type=f32))
        accf[pl.ds(i, 5)] += out[:5 * QE].reshape(5, QE, lanes)
        at = me[0] * (SX // SPC) + k + jnp.where(ph >= SPC // SPF // 2, 1, 0)
        accc[pl.ds(at, 4)] += out[5 * QE:].reshape(4, QC, lanes)
        return 0

    lax.fori_loop(0, cells, cell, 0)

    rows, cols = iota((RZ, SZ), 0), iota((RZ, SZ), 1)
    bz = weight(cols, ext_point(rows), SPF) * (SPF ** -1.5 / 24.0)
    rows, cols = iota((KZ, SZ), 0), iota((KZ, SZ), 1)
    bzc = weight(cols + me[2] * SZ, rows, SPC) * (SPC ** -1.5 / 24.0)
    zmsg[...] = jnp.zeros(zmsg.shape, f32)
    for a in range(3):
        block = accf[:, :, a * SZ:(a + 1) * SZ].reshape(EX * QE, SZ)
        tz_v[a] = nt(bz, block) + bend_v[a]
        for side in range(2):
            zmsg[side, 2 * a:2 * a + 2, :] = tz_v[a, PZ + 2 * side:PZ + 2 * side + 2, :]
        block = accc[2:2 + KX, :, a * SZ:(a + 1) * SZ].reshape(KX * QC, SZ)
        cslots[2, me[2], a * KZ:(a + 1) * KZ, :] = nt(bzc, block)

    def coarse_copy(k, d, slot):
        n = counts[k]
        return pltpu.make_async_remote_copy(
            src_ref=cslots.at[k, slot], dst_ref=cslots.at[k, slot],
            send_sem=cs_sem.at[k, d], recv_sem=cr_sem.at[k, d],
            device_id={axes[k]: lax.rem(me[k] + d, n)}, device_id_type=MESH,
        )

    def exchange(k, source, got):
        for side in range(2):
            @pl.when(has[k][side])
            def _(side=side):
                neighbour_copy(k, side, source(side), got.at[1 - side],
                               ms_sem.at[k, side], mr_sem.at[k, 1 - side]).start()
        for d in range(1, counts[k]):
            coarse_copy(k, d, me[k]).start()
        for side in range(2):
            @pl.when(has[k][side])
            def _(side=side):
                neighbour_copy(k, side, source(side), got.at[1 - side],
                               ms_sem.at[k, side], mr_sem.at[k, 1 - side]).wait_send()

            @pl.when(has[k][1 - side])
            def _(side=side):
                neighbour_copy(k, side, source(side), got.at[1 - side],
                               ms_sem.at[k, side], mr_sem.at[k, 1 - side]).wait_recv()
        for d in range(1, counts[k]):
            coarse_copy(k, d, me[k]).wait_send()
            coarse_copy(k, d, lax.rem(me[k] + counts[k] - d, counts[k])).wait_recv()
        whole = cslots[k, 0]
        for n in range(1, counts[k]):
            whole = whole + cslots[k, n]
        return whole

    whole = exchange(2, lambda side: zmsg.at[side], zgot)
    for a in range(3):
        tz_v[a, 0:2, :] = tz_v[a, 0:2, :] + zgot[0, 2 * a:2 * a + 2, :]
        tz_v[a, PZ - 2:PZ, :] = tz_v[a, PZ - 2:PZ, :] + zgot[1, 2 * a:2 * a + 2, :]
        a_v[a * PZ:(a + 1) * PZ, :] = tz_v[a, 0:PZ, :]

    cslots[1, me[1]] = whole
    whole = exchange(1, lambda side: a_v, agot)
    shape = (EX * QE, EX * PY)
    rows, cols = iota(shape, 0), iota(shape, 1)
    p_same = rows // QE == cols // PY
    q, r = rows % QE, cols % PY
    own = jnp.where(p_same & (q == r + 2), 1.0, 0.0)
    low = jnp.where(p_same & (q == r + PY + 2) & (r < 2), 1.0, 0.0)
    high = jnp.where(p_same & (q == r - (PY - 2)) & (r >= PY - 2), 1.0, 0.0)
    b_v[...] = nn(a_v[...], own) + nn(agot[0], low) + nn(agot[1], high)

    cslots[0, me[0]] = whole
    whole = exchange(0, lambda side: b_v, bgot)
    shape = (PX * PY, EX * PY)
    rows, cols = iota(shape, 0), iota(shape, 1)
    own = jnp.where(cols == rows + 2 * PY, 1.0, 0.0)
    low = jnp.where((cols == rows + (PX + 2) * PY) & (rows < 2 * PY), 1.0, 0.0)
    high = jnp.where((cols == rows - (PX - 2) * PY) & (rows >= (PX - 2) * PY), 1.0, 0.0)
    shape = (KX * QC, KX * QC)
    eye = same(iota(shape, 0), iota(shape, 1))
    for a in range(3):
        part = slice(a * PZ, (a + 1) * PZ)
        out = nt(own, b_v[part]) + nt(low, bgot[0, part]) + nt(high, bgot[1, part])
        fo_ref[a] = out.reshape(PX, PY, PZ)
        out = nt(eye, whole[a * KZ:(a + 1) * KZ]) + bendc[a]
        for p in range(KX):
            co_ref[a, p] = out[p * QC:p * QC + KY, :]


def solution(mesh):
    sizes = tuple(mesh.shape[a] for a in ("gx", "gy", "gz"))

    def step(warped, fixed, fine, coarse):
        SX, SY, SZ = warped.shape
        PX, PY, PZ = SX // SPF, SY // SPF, SZ // SPF
        KX, KY, KZ = coarse.shape[1:]
        QC = -(-KY // 8) * 8
        EX, QE, RZ = PX + 4, 16, PZ + 8
        KC = SPF * SY
        most = max(sizes)
        vmem = pl.BlockSpec(memory_space=pltpu.VMEM)
        hbm = pl.BlockSpec(memory_space=pl.ANY)
        V = pltpu.VMEM
        D = pltpu.SemaphoreType.DMA
        return pl.pallas_call(
            functools.partial(kernel, sizes),
            out_shape=(jax.ShapeDtypeStruct(fine.shape, f32),
                       jax.ShapeDtypeStruct(coarse.shape, f32)),
            in_specs=[hbm, hbm, vmem, vmem],
            out_specs=(vmem, vmem),
            scratch_shapes=[
                V((SX, SY, SZ), f32), V((SX, SY, SZ), f32),
                V((SX + 4, SY + 16, SZ), f32),
                V((2, SX, 2, SZ), f32), V((2, SX, 2, SZ), f32),
                V((2, SY, SZ), f32), V((2, SY, SZ), f32), V((2, SY, SZ), f32),
                V((2, 5 * QE, KC), bf16), V((SPC // SPF, 2, 4 * QC, KC), bf16),
                V((KC, 3 * SZ), bf16), V((KC, 3 * SZ), bf16),
                V((EX, QE, 3 * SZ), f32), V((KX + 4, QC, 3 * SZ), f32),
                V((3, RZ, EX * QE), f32), V((3, RZ, EX * QE), f32),
                V((3, KX * QC, KZ), f32), V((3, KX * QC, KZ), f32),
                V((2, 8, EX * QE), f32), V((2, 8, EX * QE), f32),
                V((3 * PZ, EX * QE), f32), V((2, 3 * PZ, EX * QE), f32),
                V((3 * PZ, EX * PY), f32), V((2, 3 * PZ, EX * PY), f32),
                V((3, most, 3 * KZ, KX * QC), f32),
                D((2, SX // SPF)), D((3, 2)), D((3, 2)), D((3, 2)), D((3, 2)),
                D((3, most)), D((3, most)),
            ],
            compiler_params=pltpu.CompilerParams(
                collective_id=0, has_side_effects=True, vmem_limit_bytes=48 * 2 ** 20
            ),
        )(warped, fixed, fine, coarse)

    in_specs = (P("gx", "gy", "gz"), P("gx", "gy", "gz"), P(None, "gx", "gy", "gz"), P())
    out_specs = (P(None, "gx", "gy", "gz"), P())
    return jax.shard_map(
        step, mesh=mesh, in_specs=in_specs, out_specs=out_specs, check_vma=False
    )
```

```python
import functools

import jax
import jax.numpy as jnp
from jax import lax
from jax.experimental import pallas as pl
from jax.experimental.pallas import tpu as pltpu
from jax.sharding import PartitionSpec as P

SPF = 8
SPC = 32
BEND = 0.01
HI = lax.Precision.HIGHEST
MESH = pl.DeviceIdType.MESH
f32 = jnp.float32
bf16 = jnp.bfloat16


def nn(a, b):
    return lax.dot_general(
        a, b, (((1,), (0,)), ((), ())), precision=HI, preferred_element_type=f32
    )


def nt(a, b):
    return lax.dot_general(
        a, b, (((1,), (1,)), ((), ())), precision=HI, preferred_element_type=f32
    )


def spline(t):
    m = jnp.abs(t)
    inner = 2.0 / 3.0 - m * m + 0.5 * m * m * m
    r = 2.0 - m
    outer = r * r * r * (1.0 / 6.0)
    return jnp.where(m < 1.0, inner, jnp.where(m < 2.0, outer, 0.0))


def weight(voxel, point, spacing):
    scaled = (2 * voxel + 1 - spacing * (2 * point + 1)).astype(f32)
    return spline(scaled * (0.5 / spacing))


def iota(shape, axis):
    return lax.broadcasted_iota(jnp.int32, shape, axis)


def diff1(out, inp):
    d = jnp.abs(out - inp)
    return jnp.where(d == 0, -2.0, jnp.where(d == 1, 1.0, 0.0)).astype(f32)


def diff2(out, inp, count):
    d = jnp.abs(out - inp)
    edge = (inp == 0) | (inp == count - 1)
    centre = jnp.where(edge, 5.0, 6.0)
    return jnp.where(
        d == 0, centre, jnp.where(d == 1, -4.0, jnp.where(d == 2, 1.0, 0.0))
    ).astype(f32)


def same(out, inp):
    return jnp.where(out == inp, 1.0, 0.0).astype(f32)


def bend_planes(px, py, qx, qy, cx, cy):
    jx, jy = same(px, qx), same(py, qy)
    tx, ty = diff1(px, qx), diff1(py, qy)
    m0 = diff2(px, qx, cx) * jy + jx * diff2(py, qy, cy) + 2.0 * tx * ty
    m1 = 2.0 * (tx * jy + jx * ty)
    return m0 * BEND, m1 * BEND, jx * jy * BEND


def kernel(sizes, w_hbm, f_hbm, fc_hbm, cc_hbm, fo_ref, co_ref,
           w_v, f_v, fc_ref, cc_ref, s_v, ysend, yrecv, zsend, zrecv, zcorr,
           wf_v, wc_v, fh_v, fl_v,
           accf, accc, tz_v, bend_v, ccp, bendc, zmsg, zgot, a_v, agot, b_v, bgot,
           cslots, load_sem, small_sem, hs_sem, hr_sem, ys_sem, yr_sem,
           ms_sem, mr_sem, cs_sem, cr_sem):
    nx, ny, nz = sizes
    axes = ("gx", "gy", "gz")
    counts = sizes
    me = [lax.axis_index(a) for a in axes]
    SX, SY, SZ = w_v.shape
    PX, PY, PZ = SX // SPF, SY // SPF, SZ // SPF
    KX, KY, KZ = cc_ref.shape[1:]
    EX, QE, QC = PX + 4, 2 * PY, accc.shape[1]
    cells = SX // SPF
    lanes = 3 * SZ

    loads = []
    for c in range(cells):
        part = pl.ds(c * SPF, SPF)
        loads.append((
            pltpu.make_async_copy(w_hbm.at[part], w_v.at[part], load_sem.at[0, c]),
            pltpu.make_async_copy(f_hbm.at[part], f_v.at[part], load_sem.at[1, c]),
        ))
    small = (pltpu.make_async_copy(fc_hbm, fc_ref, small_sem.at[0]),
             pltpu.make_async_copy(cc_hbm, cc_ref, small_sem.at[1]))
    order = [0, cells - 1] + list(range(1, cells - 1))
    for c in order:
        loads[c][0].start()
        loads[c][1].start()
    for copy in small:
        copy.start()

    zero_plane = jnp.zeros((2, SY, SZ), f32)
    s_v[0:2, 8:8 + SY, :] = zero_plane
    s_v[SX + 2:SX + 4, 8:8 + SY, :] = zero_plane
    yrecv[...] = jnp.zeros(yrecv.shape, f32)
    zrecv[...] = jnp.zeros(zrecv.shape, f32)
    zgot[...] = jnp.zeros(zgot.shape, f32)
    agot[...] = jnp.zeros(agot.shape, f32)
    bgot[...] = jnp.zeros(bgot.shape, f32)

    barrier = pltpu.get_barrier_semaphore()
    total = 0
    for k, a in enumerate(axes):
        for d in range(1, counts[k]):
            pl.semaphore_signal(
                barrier, inc=1, device_id={a: lax.rem(me[k] + d, counts[k])}, device_id_type=MESH
            )
            total += 1

    def split_store(ref, index, value):
        high = value.astype(bf16)
        ref[index + (0,)] = high
        ref[index + (1,)] = (value - high.astype(f32)).astype(bf16)

    KC = SPF * SY
    def ext_q(q):
        return jnp.where(q < PY, q, jnp.where(q < PY + 2, q - PY - 2, q - 2))

    rows, cols = iota((5 * QE, KC), 0), iota((5 * QE, KC), 1)
    split_store(wf_v, (), weight(cols // SY, rows // QE - 2, SPF)
                * weight(cols % SY, ext_q(rows % QE), SPF))
    rows, cols = iota((4 * QC, KC), 0), iota((4 * QC, KC), 1)
    along_y = weight(cols % SY + me[1] * SY, rows % QC, SPC)
    for ph in range(SPC // SPF):
        first = -2 if ph < SPC // SPF // 2 else -1
        split_store(wc_v, (ph,),
                    weight(cols // SY + ph * SPF, rows // QC + first, SPC) * along_y)

    pl.semaphore_wait(barrier, total)

    has = [(me[k] > 0, me[k] < counts[k] - 1) for k in range(3)]
    pieces = ys_sem.shape[1]
    each = SX // pieces

    def halo(k, side, piece=0):
        if k == 1:
            part = pl.ds(piece * each, each)
            return neighbour_copy(
                k, side, ysend.at[side, part], yrecv.at[1 - side, part],
                ys_sem.at[side, piece], yr_sem.at[1 - side, piece])
        if k == 0:
            src = s_v.at[pl.ds(2 if side == 0 else SX, 2), pl.ds(8, SY), :]
            dst = s_v.at[pl.ds(SX + 2 if side == 0 else 0, 2), pl.ds(8, SY), :]
        else:
            src, dst = zsend.at[side], zrecv.at[1 - side]
        return neighbour_copy(k, side, src, dst, hs_sem.at[k, side], hr_sem.at[k, 1 - side])

    def neighbour_copy(k, side, src, dst, send, recv):
        other = me[k] - 1 if side == 0 else me[k] + 1
        return pltpu.make_async_remote_copy(
            src_ref=src, dst_ref=dst, send_sem=send, recv_sem=recv,
            device_id={axes[k]: other}, device_id_type=MESH,
        )

    def start_halo(k, side, piece=0):
        @pl.when(has[k][side])
        def _():
            halo(k, side, piece).start()

    lane = iota((SY, SZ), 1)

    def one_slab(x, carry):
        low, high = carry
        s = w_v[x] + f_v[x]
        s_v[x + 2, 8:8 + SY, :] = s
        ysend[0, x] = s[0:2]
        ysend[1, x] = s[SY - 2:SY]
        here = lane // 2 == x
        low = jnp.where(here, pltpu.roll(s, 2 * x, 1), low)
        high = jnp.where(here, pltpu.roll(s, lax.rem(2 * x + 2, SZ), 1), high)
        return low, high

    carry = (jnp.zeros((SY, SZ), f32), jnp.zeros((SY, SZ), f32))
    done = set()
    sent = set()
    for c in order:
        for copy in loads[c]:
            copy.wait()
        carry = lax.fori_loop(c * SPF, (c + 1) * SPF, one_slab, carry)
        done.add(c)
        for piece in range(pieces):
            inside = range(piece * each // SPF, (piece + 1) * each // SPF)
            if piece not in sent and all(n in done for n in inside):
                sent.add(piece)
                start_halo(1, 0, piece)
                start_halo(1, 1, piece)
        if c == 0:
            start_halo(0, 0)
        if c == cells - 1:
            start_halo(0, 1)
    zsend[0] = carry[0]
    zsend[1] = carry[1]
    start_halo(2, 0)
    start_halo(2, 1)

    accf[...] = jnp.zeros(accf.shape, f32)
    accc[...] = jnp.zeros(accc.shape, f32)
    for copy in small:
        copy.wait()
    shape = (EX * QE, PX * PY)
    rows, cols = iota(shape, 0), iota(shape, 1)
    ox, oy = me[0] * PX, me[1] * PY
    outer, inner = rows // (EX * PY), rows % (EX * PY)
    planes = bend_planes(inner // PY - 2 + ox, ext_q(inner % PY + PY * outer) + oy,
                         cols // PY + ox, cols % PY + oy, PX * nx, PY * ny)
    RZ = tz_v.shape[2]

    def ext_point(row):
        return jnp.where(row < PZ, row, jnp.where(row < PZ + 2, row - PZ - 2, row - 2))

    oz = me[2] * PZ
    zr, zc = ext_point(iota((RZ, PZ), 0)) + oz, iota((RZ, PZ), 1) + oz
    along = (same(zr, zc), diff1(zr, zc), diff2(zr, zc, PZ * nz))
    for a in range(3):
        block = fc_ref[a].reshape(PX * PY, PZ)
        factors = [nn(plane, block) for plane in planes]
        for half in range(2):
            part = slice(half * EX * PY, (half + 1) * EX * PY)
            bend_v[half, a] = (nt(along[0], factors[0][part]) + nt(along[1], factors[1][part])
                               + nt(along[2], factors[2][part]))
    shape = (KX * QC, KX * QC)
    rows, cols = iota(shape, 0), iota(shape, 1)
    planes = bend_planes(rows // QC, rows % QC, cols // QC, cols % QC, KX, KY)
    zr, zc = iota((KZ, KZ), 0), iota((KZ, KZ), 1)
    for a in range(3):
        for p in range(KX):
            ccp[a, p * QC:p * QC + KY, :] = cc_ref[a, p]
        block = ccp[a]
        bendc[a] = (nn(planes[0], block) + nn(planes[1], nn(block, diff1(zr, zc)))
                    + BEND * nn(block, diff2(zr, zc, KZ)))

    for k in (0, 1, 2):
        for side in range(2):
            for piece in range(pieces if k == 1 else 1):
                @pl.when(has[k][side])
                def _(k=k, side=side, piece=piece):
                    halo(k, side, piece).wait_send()

                @pl.when(has[k][1 - side])
                def _(k=k, side=side, piece=piece):
                    halo(k, side, piece).wait_recv()

    even = lane % 2 == 0
    dl = zrecv[0] - zsend[1]
    dh = zrecv[1] - zsend[0]
    zcorr[0] = jnp.where(even, dl - 8.0 * pltpu.roll(dl, SZ - 1, 1), dl)
    zcorr[1] = jnp.where(even, -dh, 8.0 * pltpu.roll(dh, 1, 1) - dh)

    def forces(i):
        slot = i % 2
        for xx in range(SPF):
            x = i * SPF + xx
            s_v[x + 2, 6:8, :] = yrecv[0, x]
            s_v[x + 2, 8 + SY:10 + SY, :] = yrecv[1, x]
            d = w_v[x] - f_v[x]
            s = s_v[x + 2, 8:8 + SY, :]
            gx = (s_v[x, 8:8 + SY, :] - s_v[x + 4, 8:8 + SY, :]
                  + 8.0 * (s_v[x + 3, 8:8 + SY, :] - s_v[x + 1, 8:8 + SY, :]))
            gy = (s_v[x + 2, 6:6 + SY, :] - s_v[x + 2, 10:10 + SY, :]
                  + 8.0 * (s_v[x + 2, 9:9 + SY, :] - s_v[x + 2, 7:7 + SY, :]))
            gz = (pltpu.roll(s, 2, 1) - pltpu.roll(s, SZ - 2, 1)
                  + 8.0 * (pltpu.roll(s, SZ - 1, 1) - pltpu.roll(s, 1, 1)))
            corr = jnp.where(lane < 2, pltpu.roll(zcorr[0], (SZ - 2 * x) % SZ, 1), 0.0)
            corr = jnp.where(lane >= SZ - 2,
                             pltpu.roll(zcorr[1], (2 * SZ - 2 - 2 * x) % SZ, 1), corr)
            gz = gz + corr
            for a, g in enumerate((gx, gy, gz)):
                force = g * d
                high = force.astype(bf16)
                fh_v[slot, xx * SY:(xx + 1) * SY, a * SZ:(a + 1) * SZ] = high
                fl_v[slot, xx * SY:(xx + 1) * SY, a * SZ:(a + 1) * SZ] = (
                    force - high.astype(f32)).astype(bf16)

    def gather(i):
        slot = i % 2
        k, ph = divmod(i, SPC // SPF)
        many = 5 * QE + 4 * QC
        weights = jnp.concatenate([wf_v[0], wc_v[ph, 0], wf_v[1], wc_v[ph, 1]], axis=0)
        both = jnp.dot(weights, fh_v[slot], preferred_element_type=f32)
        out = both[:many] + both[many:] + jnp.dot(
            weights[:many], fl_v[slot], preferred_element_type=f32)
        fine = out[:5 * QE].reshape(5, 2, PY, lanes)
        accf[0, i:i + 5] += fine[:, 0]
        accf[1, i:i + 5] += fine[:, 1]
        at = me[0] * (SX // SPC) + k + (1 if ph >= SPC // SPF // 2 else 0)
        accc[pl.ds(at, 4)] += out[5 * QE:].reshape(4, QC, lanes)

    forces(0)
    for i in range(cells):
        if i + 1 < cells:
            forces(i + 1)
        gather(i)

    rows, cols = iota((RZ, SZ), 0), iota((RZ, SZ), 1)
    bz = weight(cols, ext_point(rows), SPF) * (SPF ** -1.5 / 24.0)
    rows, cols = iota((KZ, SZ), 0), iota((KZ, SZ), 1)
    bzc = weight(cols + me[2] * SZ, rows, SPC) * (SPC ** -1.5 / 24.0)
    for a in range(3):
        for half in range(2):
            block = accf[half, :, :, a * SZ:(a + 1) * SZ].reshape(EX * PY, SZ)
            tz_v[half, a] = nt(bz, block) + bend_v[half, a]
            for side in range(2):
                zmsg[side, half, 2 * a:2 * a + 2, :] = tz_v[
                    half, a, PZ + 2 * side:PZ + 2 * side + 2, :]
    blocks = [accc[2:2 + KX, :, a * SZ:(a + 1) * SZ].reshape(KX * QC, SZ) for a in range(3)]
    cslots[2, me[2]] = nt(bzc, jnp.concatenate(blocks, axis=0))

    def coarse_copy(k, d, slot):
        n = counts[k]
        return pltpu.make_async_remote_copy(
            src_ref=cslots.at[k, slot], dst_ref=cslots.at[k, slot],
            send_sem=cs_sem.at[k, d], recv_sem=cr_sem.at[k, d],
            device_id={axes[k]: lax.rem(me[k] + d, n)}, device_id_type=MESH,
        )

    def exchange(k, source, got):
        for side in range(2):
            @pl.when(has[k][side])
            def _(side=side):
                neighbour_copy(k, side, source(side), got.at[1 - side],
                               ms_sem.at[k, side], mr_sem.at[k, 1 - side]).start()
        for d in range(1, counts[k]):
            coarse_copy(k, d, me[k]).start()
        for side in range(2):
            @pl.when(has[k][side])
            def _(side=side):
                neighbour_copy(k, side, source(side), got.at[1 - side],
                               ms_sem.at[k, side], mr_sem.at[k, 1 - side]).wait_send()

            @pl.when(has[k][1 - side])
            def _(side=side):
                neighbour_copy(k, side, source(side), got.at[1 - side],
                               ms_sem.at[k, side], mr_sem.at[k, 1 - side]).wait_recv()
        for d in range(1, counts[k]):
            coarse_copy(k, d, me[k]).wait_send()
            coarse_copy(k, d, lax.rem(me[k] + counts[k] - d, counts[k])).wait_recv()
        whole = cslots[k, 0]
        for n in range(1, counts[k]):
            whole = whole + cslots[k, n]
        return whole

    whole = exchange(2, lambda side: zmsg.at[side], zgot)
    for half in range(2):
        for a in range(3):
            tz_v[half, a, 0:2, :] = tz_v[half, a, 0:2, :] + zgot[0, half, 2 * a:2 * a + 2, :]
            tz_v[half, a, PZ - 2:PZ, :] = (
                tz_v[half, a, PZ - 2:PZ, :] + zgot[1, half, 2 * a:2 * a + 2, :])
            a_v[half, a * PZ:(a + 1) * PZ, :] = tz_v[half, a, 0:PZ, :]

    cslots[1, me[1]] = whole
    whole = exchange(1, lambda side: a_v.at[1], agot)
    shape = (EX * PY, EX * PY)
    rows, cols = iota(shape, 0), iota(shape, 1)
    p_same = rows // PY == cols // PY
    q, r = rows % PY, cols % PY
    low = jnp.where(p_same & (q == r + 2) & (r < 2), 1.0, 0.0)
    high = jnp.where(p_same & (q == r - (PY - 2)) & (r >= PY - 2), 1.0, 0.0)
    b_v[...] = a_v[0] + nn(agot[0], low) + nn(agot[1], high)

    cslots[0, me[0]] = whole
    whole = exchange(0, lambda side: b_v, bgot)
    shape = (PX * PY, EX * PY)
    rows, cols = iota(shape, 0), iota(shape, 1)
    own = jnp.where(cols == rows + 2 * PY, 1.0, 0.0)
    low = jnp.where((cols == rows + (PX + 2) * PY) & (rows < 2 * PY), 1.0, 0.0)
    high = jnp.where((cols == rows - (PX - 2) * PY) & (rows >= (PX - 2) * PY), 1.0, 0.0)
    shape = (3 * KX * QC, 3 * KX * QC)
    turned = nt(same(iota(shape, 0), iota(shape, 1)), whole)
    for a in range(3):
        part = slice(a * PZ, (a + 1) * PZ)
        out = nt(own, b_v[part]) + nt(low, bgot[0, part]) + nt(high, bgot[1, part])
        fo_ref[a] = out.reshape(PX, PY, PZ)
        out = turned[a * KX * QC:(a + 1) * KX * QC] + bendc[a]
        for p in range(KX):
            co_ref[a, p] = out[p * QC:p * QC + KY, :]


def solution(mesh):
    sizes = tuple(mesh.shape[a] for a in ("gx", "gy", "gz"))

    def step(warped, fixed, fine, coarse):
        SX, SY, SZ = warped.shape
        PX, PY, PZ = SX // SPF, SY // SPF, SZ // SPF
        KX, KY, KZ = coarse.shape[1:]
        QC = KY
        EX, QE, RZ = PX + 4, 2 * PY, PZ + 8
        KC = SPF * SY
        most = max(sizes)
        vmem = pl.BlockSpec(memory_space=pltpu.VMEM)
        hbm = pl.BlockSpec(memory_space=pltpu.HBM)
        V = pltpu.VMEM
        D = pltpu.SemaphoreType.DMA
        return pl.pallas_call(
            functools.partial(kernel, sizes),
            out_shape=(jax.ShapeDtypeStruct(fine.shape, f32),
                       jax.ShapeDtypeStruct(coarse.shape, f32)),
            in_specs=[hbm] * 4,
            out_specs=(vmem, vmem),
            scratch_shapes=[
                V((SX, SY, SZ), f32), V((SX, SY, SZ), f32),
                V((3, PX, PY, PZ), f32), V(coarse.shape, f32),
                V((SX + 4, SY + 16, SZ), f32),
                V((2, SX, 2, SZ), f32), V((2, SX, 2, SZ), f32),
                V((2, SY, SZ), f32), V((2, SY, SZ), f32), V((2, SY, SZ), f32),
                V((2, 5 * QE, KC), bf16), V((SPC // SPF, 2, 4 * QC, KC), bf16),
                V((2, KC, 3 * SZ), bf16), V((2, KC, 3 * SZ), bf16),
                V((2, EX, PY, 3 * SZ), f32), V((KX + 4, QC, 3 * SZ), f32),
                V((2, 3, RZ, EX * PY), f32), V((2, 3, RZ, EX * PY), f32),
                V((3, KX * QC, KZ), f32), V((3, KX * QC, KZ), f32),
                V((2, 2, 8, EX * PY), f32), V((2, 2, 8, EX * PY), f32),
                V((2, 3 * PZ, EX * PY), f32), V((2, 3 * PZ, EX * PY), f32),
                V((3 * PZ, EX * PY), f32), V((2, 3 * PZ, EX * PY), f32),
                V((3, most, KZ, 3 * KX * QC), f32),
                D((2, SX // SPF)), D((2,)), D((3, 2)), D((3, 2)), D((2, 4)), D((2, 4)),
                D((3, 2)), D((3, 2)), D((3, most)), D((3, most)),
            ],
            compiler_params=pltpu.CompilerParams(
                collective_id=0, has_side_effects=True, vmem_limit_bytes=48 * 2 ** 20
            ),
        )(warped, fixed, fine, coarse)

    in_specs = (P("gx", "gy", "gz"), P("gx", "gy", "gz"), P(None, "gx", "gy", "gz"), P())
    out_specs = (P(None, "gx", "gy", "gz"), P())
    return jax.shard_map(
        step, mesh=mesh, in_specs=in_specs, out_specs=out_specs, check_vma=False
    )
```

```python
import functools

import jax
import jax.numpy as jnp
from jax import lax
from jax.experimental import pallas as pl
from jax.experimental.pallas import tpu as pltpu
from jax.sharding import PartitionSpec as P

SPF = 8
SPC = 32
BEND = 0.01
HI = lax.Precision.HIGHEST
MESH = pl.DeviceIdType.MESH
f32 = jnp.float32
bf16 = jnp.bfloat16


def nn(a, b):
    return lax.dot_general(
        a, b, (((1,), (0,)), ((), ())), precision=HI, preferred_element_type=f32
    )


def nt(a, b):
    return lax.dot_general(
        a, b, (((1,), (1,)), ((), ())), precision=HI, preferred_element_type=f32
    )


def spline(t):
    m = jnp.abs(t)
    inner = 2.0 / 3.0 - m * m + 0.5 * m * m * m
    r = 2.0 - m
    outer = r * r * r * (1.0 / 6.0)
    return jnp.where(m < 1.0, inner, jnp.where(m < 2.0, outer, 0.0))


def weight(voxel, point, spacing):
    scaled = (2 * voxel + 1 - spacing * (2 * point + 1)).astype(f32)
    return spline(scaled * (0.5 / spacing))


def iota(shape, axis):
    return lax.broadcasted_iota(jnp.int32, shape, axis)


def diff1(out, inp):
    d = jnp.abs(out - inp)
    return jnp.where(d == 0, -2.0, jnp.where(d == 1, 1.0, 0.0)).astype(f32)


def diff2(out, inp, count):
    d = jnp.abs(out - inp)
    edge = (inp == 0) | (inp == count - 1)
    centre = jnp.where(edge, 5.0, 6.0)
    return jnp.where(
        d == 0, centre, jnp.where(d == 1, -4.0, jnp.where(d == 2, 1.0, 0.0))
    ).astype(f32)


def same(out, inp):
    return jnp.where(out == inp, 1.0, 0.0).astype(f32)


def bend_planes(px, py, qx, qy, cx, cy):
    jx, jy = same(px, qx), same(py, qy)
    tx, ty = diff1(px, qx), diff1(py, qy)
    m0 = diff2(px, qx, cx) * jy + jx * diff2(py, qy, cy) + 2.0 * tx * ty
    m1 = 2.0 * (tx * jy + jx * ty)
    return m0 * BEND, m1 * BEND, jx * jy * BEND


def kernel(sizes, w_hbm, f_hbm, fc_hbm, cc_hbm, fo_ref, co_ref,
           w_v, f_v, fc_ref, cc_ref, s_v, ysend, yrecv, zsend, zrecv, zcorr,
           wf_v, wc_v, fh_v, fl_v,
           accf, accc, tz_v, bend_v, ccp, bendc, zmsg, zgot, a_v, agot, b_v, bgot,
           cslots, load_sem, small_sem, hs_sem, hr_sem, ys_sem, yr_sem,
           ms_sem, mr_sem, cs_sem, cr_sem):
    nx, ny, nz = sizes
    axes = ("gx", "gy", "gz")
    counts = sizes
    me = [lax.axis_index(a) for a in axes]
    SX, SY, SZ = w_v.shape
    PX, PY, PZ = SX // SPF, SY // SPF, SZ // SPF
    KX, KY, KZ = cc_ref.shape[1:]
    EX, QE, QC = PX + 4, 2 * PY, accc.shape[1]
    cells = SX // SPF
    lanes = 3 * SZ

    loads = []
    for c in range(cells):
        part = pl.ds(c * SPF, SPF)
        loads.append((
            pltpu.make_async_copy(w_hbm.at[part], w_v.at[part], load_sem.at[0, c]),
            pltpu.make_async_copy(f_hbm.at[part], f_v.at[part], load_sem.at[1, c]),
        ))
    small = (pltpu.make_async_copy(fc_hbm, fc_ref, small_sem.at[0]),
             pltpu.make_async_copy(cc_hbm, cc_ref, small_sem.at[1]))
    order = [0, cells - 1] + list(range(1, cells - 1))
    for c in order:
        loads[c][0].start()
        loads[c][1].start()
    for copy in small:
        copy.start()

    zero_plane = jnp.zeros((2, SY, SZ), f32)
    s_v[0:2, 8:8 + SY, :] = zero_plane
    s_v[SX + 2:SX + 4, 8:8 + SY, :] = zero_plane
    yrecv[...] = jnp.zeros(yrecv.shape, f32)
    zrecv[...] = jnp.zeros(zrecv.shape, f32)
    zgot[...] = jnp.zeros(zgot.shape, f32)
    agot[...] = jnp.zeros(agot.shape, f32)
    bgot[...] = jnp.zeros(bgot.shape, f32)

    barrier = pltpu.get_barrier_semaphore()
    total = 0
    for k, a in enumerate(axes):
        for d in range(1, counts[k]):
            pl.semaphore_signal(
                barrier, inc=1, device_id={a: lax.rem(me[k] + d, counts[k])}, device_id_type=MESH
            )
            total += 1

    def split_store(ref, index, value):
        high = value.astype(bf16)
        ref[index + (0,)] = high
        ref[index + (1,)] = (value - high.astype(f32)).astype(bf16)

    KC = SPF * SY
    def ext_q(q):
        return jnp.where(q < PY, q, jnp.where(q < PY + 2, q - PY - 2, q - 2))

    rows, cols = iota((5 * QE, KC), 0), iota((5 * QE, KC), 1)
    split_store(wf_v, (), weight(cols // SY, rows // QE - 2, SPF)
                * weight(cols % SY, ext_q(rows % QE), SPF))
    rows, cols = iota((4 * QC, KC), 0), iota((4 * QC, KC), 1)
    along_y = weight(cols % SY + me[1] * SY, rows % QC, SPC)
    for ph in range(SPC // SPF):
        first = -2 if ph < SPC // SPF // 2 else -1
        split_store(wc_v, (ph,),
                    weight(cols // SY + ph * SPF, rows // QC + first, SPC) * along_y)

    pl.semaphore_wait(barrier, total)

    has = [(me[k] > 0, me[k] < counts[k] - 1) for k in range(3)]
    pieces = ys_sem.shape[1]
    each = SX // pieces

    def halo(k, side, piece=0):
        if k == 1:
            part = pl.ds(piece * each, each)
            return neighbour_copy(
                k, side, ysend.at[side, part], yrecv.at[1 - side, part],
                ys_sem.at[side, piece], yr_sem.at[1 - side, piece])
        if k == 0:
            src = s_v.at[pl.ds(2 if side == 0 else SX, 2), pl.ds(8, SY), :]
            dst = s_v.at[pl.ds(SX + 2 if side == 0 else 0, 2), pl.ds(8, SY), :]
        else:
            src, dst = zsend.at[side], zrecv.at[1 - side]
        return neighbour_copy(k, side, src, dst, hs_sem.at[k, side], hr_sem.at[k, 1 - side])

    def neighbour_copy(k, side, src, dst, send, recv):
        other = me[k] - 1 if side == 0 else me[k] + 1
        return pltpu.make_async_remote_copy(
            src_ref=src, dst_ref=dst, send_sem=send, recv_sem=recv,
            device_id={axes[k]: other}, device_id_type=MESH,
        )

    def start_halo(k, side, piece=0):
        @pl.when(has[k][side])
        def _():
            halo(k, side, piece).start()

    lane = iota((SY, SZ), 1)

    def one_slab(x, carry):
        low, high = carry
        s = w_v[x] + f_v[x]
        s_v[x + 2, 8:8 + SY, :] = s
        ysend[0, x] = s[0:2]
        ysend[1, x] = s[SY - 2:SY]
        here = lane // 2 == x
        low = jnp.where(here, pltpu.roll(s, 2 * x, 1), low)
        high = jnp.where(here, pltpu.roll(s, lax.rem(2 * x + 2, SZ), 1), high)
        return low, high

    carry = (jnp.zeros((SY, SZ), f32), jnp.zeros((SY, SZ), f32))
    done = set()
    sent = set()
    for c in order:
        for copy in loads[c]:
            copy.wait()
        carry = lax.fori_loop(c * SPF, (c + 1) * SPF, one_slab, carry)
        done.add(c)
        for piece in range(pieces):
            inside = range(piece * each // SPF, (piece + 1) * each // SPF)
            if piece not in sent and all(n in done for n in inside):
                sent.add(piece)
                start_halo(1, 0, piece)
                start_halo(1, 1, piece)
        if c == 0:
            start_halo(0, 0)
        if c == cells - 1:
            start_halo(0, 1)
    zsend[0] = carry[0]
    zsend[1] = carry[1]
    start_halo(2, 0)
    start_halo(2, 1)

    accf[...] = jnp.zeros(accf.shape, f32)
    accc[...] = jnp.zeros(accc.shape, f32)
    for copy in small:
        copy.wait()
    shape = (EX * QE, PX * PY)
    rows, cols = iota(shape, 0), iota(shape, 1)
    ox, oy = me[0] * PX, me[1] * PY
    outer, inner = rows // (EX * PY), rows % (EX * PY)
    planes = bend_planes(inner // PY - 2 + ox, ext_q(inner % PY + PY * outer) + oy,
                         cols // PY + ox, cols % PY + oy, PX * nx, PY * ny)
    RZ = tz_v.shape[2]

    def ext_point(row):
        return jnp.where(row < PZ, row, jnp.where(row < PZ + 2, row - PZ - 2, row - 2))

    oz = me[2] * PZ
    zr, zc = ext_point(iota((RZ, PZ), 0)) + oz, iota((RZ, PZ), 1) + oz
    along = (same(zr, zc), diff1(zr, zc), diff2(zr, zc, PZ * nz))
    for a in range(3):
        block = fc_ref[a].reshape(PX * PY, PZ)
        factors = [nn(plane, block) for plane in planes]
        for half in range(2):
            part = slice(half * EX * PY, (half + 1) * EX * PY)
            bend_v[half, a] = (nt(along[0], factors[0][part]) + nt(along[1], factors[1][part])
                               + nt(along[2], factors[2][part]))
    shape = (KX * QC, KX * QC)
    rows, cols = iota(shape, 0), iota(shape, 1)
    planes = bend_planes(rows // QC, rows % QC, cols // QC, cols % QC, KX, KY)
    zr, zc = iota((KZ, KZ), 0), iota((KZ, KZ), 1)
    for a in range(3):
        for p in range(KX):
            ccp[a, p * QC:p * QC + KY, :] = cc_ref[a, p]
        block = ccp[a]
        bendc[a] = (nn(planes[0], block) + nn(planes[1], nn(block, diff1(zr, zc)))
                    + BEND * nn(block, diff2(zr, zc, KZ)))

    for k in (0, 1, 2):
        for side in range(2):
            for piece in range(pieces if k == 1 else 1):
                @pl.when(has[k][side])
                def _(k=k, side=side, piece=piece):
                    halo(k, side, piece).wait_send()

                @pl.when(has[k][1 - side])
                def _(k=k, side=side, piece=piece):
                    halo(k, side, piece).wait_recv()

    even = lane % 2 == 0
    dl = zrecv[0] - zsend[1]
    dh = zrecv[1] - zsend[0]
    zcorr[0] = jnp.where(even, dl - 8.0 * pltpu.roll(dl, SZ - 1, 1), dl)
    zcorr[1] = jnp.where(even, -dh, 8.0 * pltpu.roll(dh, 1, 1) - dh)

    def forces(i):
        slot = i % 2
        for xx in range(SPF):
            x = i * SPF + xx
            s_v[x + 2, 6:8, :] = yrecv[0, x]
            s_v[x + 2, 8 + SY:10 + SY, :] = yrecv[1, x]
            d = w_v[x] - f_v[x]
            s = s_v[x + 2, 8:8 + SY, :]
            gx = (s_v[x, 8:8 + SY, :] - s_v[x + 4, 8:8 + SY, :]
                  + 8.0 * (s_v[x + 3, 8:8 + SY, :] - s_v[x + 1, 8:8 + SY, :]))
            gy = (s_v[x + 2, 6:6 + SY, :] - s_v[x + 2, 10:10 + SY, :]
                  + 8.0 * (s_v[x + 2, 9:9 + SY, :] - s_v[x + 2, 7:7 + SY, :]))
            gz = (pltpu.roll(s, 2, 1) - pltpu.roll(s, SZ - 2, 1)
                  + 8.0 * (pltpu.roll(s, SZ - 1, 1) - pltpu.roll(s, 1, 1)))
            corr = jnp.where(lane < 2, pltpu.roll(zcorr[0], (SZ - 2 * x) % SZ, 1), 0.0)
            corr = jnp.where(lane >= SZ - 2,
                             pltpu.roll(zcorr[1], (2 * SZ - 2 - 2 * x) % SZ, 1), corr)
            gz = gz + corr
            for a, g in enumerate((gx, gy, gz)):
                force = g * d
                high = force.astype(bf16)
                fh_v[slot, xx * SY:(xx + 1) * SY, a * SZ:(a + 1) * SZ] = high
                fl_v[slot, xx * SY:(xx + 1) * SY, a * SZ:(a + 1) * SZ] = (
                    force - high.astype(f32)).astype(bf16)

    def gather(i):
        slot = i % 2
        k, ph = divmod(i, SPC // SPF)
        many = 5 * QE + 4 * QC
        weights = jnp.concatenate([wf_v[0], wc_v[ph, 0], wf_v[1], wc_v[ph, 1]], axis=0)
        both = jnp.dot(weights, fh_v[slot], preferred_element_type=f32)
        out = both[:many] + both[many:] + jnp.dot(
            weights[:many], fl_v[slot], preferred_element_type=f32)
        fine = out[:5 * QE].reshape(5, 2, PY, lanes)
        accf[0, i:i + 5] += fine[:, 0]
        accf[1, i:i + 5] += fine[:, 1]
        at = me[0] * (SX // SPC) + k + (1 if ph >= SPC // SPF // 2 else 0)
        accc[pl.ds(at, 4)] += out[5 * QE:].reshape(4, QC, lanes)

    forces(0)
    for i in range(cells):
        if i + 1 < cells:
            forces(i + 1)
        gather(i)

    rows, cols = iota((RZ, SZ), 0), iota((RZ, SZ), 1)
    bz = weight(cols, ext_point(rows), SPF) * (SPF ** -1.5 / 24.0)
    rows, cols = iota((KZ, SZ), 0), iota((KZ, SZ), 1)
    bzc = weight(cols + me[2] * SZ, rows, SPC) * (SPC ** -1.5 / 24.0)
    for a in range(3):
        for half in range(2):
            block = accf[half, :, :, a * SZ:(a + 1) * SZ].reshape(EX * PY, SZ)
            tz_v[half, a] = nt(bz, block) + bend_v[half, a]
            for side in range(2):
                zmsg[side, half, 2 * a:2 * a + 2, :] = tz_v[
                    half, a, PZ + 2 * side:PZ + 2 * side + 2, :]
    blocks = [accc[2:2 + KX, :, a * SZ:(a + 1) * SZ].reshape(KX * QC, SZ) for a in range(3)]
    cslots[2, me[2]] = nt(bzc, jnp.concatenate(blocks, axis=0))

    def coarse_copy(k, d, slot):
        n = counts[k]
        return pltpu.make_async_remote_copy(
            src_ref=cslots.at[k, slot], dst_ref=cslots.at[k, slot],
            send_sem=cs_sem.at[k, d], recv_sem=cr_sem.at[k, d],
            device_id={axes[k]: lax.rem(me[k] + d, n)}, device_id_type=MESH,
        )

    def exchange(k, source, got):
        for side in range(2):
            @pl.when(has[k][side])
            def _(side=side):
                neighbour_copy(k, side, source(side), got.at[1 - side],
                               ms_sem.at[k, side], mr_sem.at[k, 1 - side]).start()
        for d in range(1, counts[k]):
            coarse_copy(k, d, me[k]).start()
        for side in range(2):
            @pl.when(has[k][side])
            def _(side=side):
                neighbour_copy(k, side, source(side), got.at[1 - side],
                               ms_sem.at[k, side], mr_sem.at[k, 1 - side]).wait_send()

            @pl.when(has[k][1 - side])
            def _(side=side):
                neighbour_copy(k, side, source(side), got.at[1 - side],
                               ms_sem.at[k, side], mr_sem.at[k, 1 - side]).wait_recv()
        for d in range(1, counts[k]):
            coarse_copy(k, d, me[k]).wait_send()
            coarse_copy(k, d, lax.rem(me[k] + counts[k] - d, counts[k])).wait_recv()
        whole = cslots[k, 0]
        for n in range(1, counts[k]):
            whole = whole + cslots[k, n]
        return whole

    whole = exchange(2, lambda side: zmsg.at[side], zgot)
    for half in range(2):
        for a in range(3):
            tz_v[half, a, 0:2, :] = tz_v[half, a, 0:2, :] + zgot[0, half, 2 * a:2 * a + 2, :]
            tz_v[half, a, PZ - 2:PZ, :] = (
                tz_v[half, a, PZ - 2:PZ, :] + zgot[1, half, 2 * a:2 * a + 2, :])
            a_v[half, a * PZ:(a + 1) * PZ, :] = tz_v[half, a, 0:PZ, :]

    cslots[1, me[1]] = whole
    whole = exchange(1, lambda side: a_v.at[1], agot)
    shape = (EX * PY, EX * PY)
    rows, cols = iota(shape, 0), iota(shape, 1)
    p_same = rows // PY == cols // PY
    q, r = rows % PY, cols % PY
    low = jnp.where(p_same & (q == r + 2) & (r < 2), 1.0, 0.0)
    high = jnp.where(p_same & (q == r - (PY - 2)) & (r >= PY - 2), 1.0, 0.0)
    b_v[...] = a_v[0] + nn(agot[0], low) + nn(agot[1], high)

    cslots[0, me[0]] = whole
    whole = exchange(0, lambda side: b_v, bgot)
    shape = (PX * PY, EX * PY)
    rows, cols = iota(shape, 0), iota(shape, 1)
    own = jnp.where(cols == rows + 2 * PY, 1.0, 0.0)
    low = jnp.where((cols == rows + (PX + 2) * PY) & (rows < 2 * PY), 1.0, 0.0)
    high = jnp.where((cols == rows - (PX - 2) * PY) & (rows >= (PX - 2) * PY), 1.0, 0.0)
    shape = (3 * KX * QC, 3 * KX * QC)
    turned = nt(same(iota(shape, 0), iota(shape, 1)), whole)
    for a in range(3):
        part = slice(a * PZ, (a + 1) * PZ)
        out = nt(own, b_v[part]) + nt(low, bgot[0, part]) + nt(high, bgot[1, part])
        fo_ref[a] = out.reshape(PX, PY, PZ)
        out = turned[a * KX * QC:(a + 1) * KX * QC] + bendc[a]
        for p in range(KX):
            co_ref[a, p] = out[p * QC:p * QC + KY, :]


def solution(mesh):
    sizes = tuple(mesh.shape[a] for a in ("gx", "gy", "gz"))

    def step(warped, fixed, fine, coarse):
        SX, SY, SZ = warped.shape
        PX, PY, PZ = SX // SPF, SY // SPF, SZ // SPF
        KX, KY, KZ = coarse.shape[1:]
        QC = KY
        EX, QE, RZ = PX + 4, 2 * PY, PZ + 8
        KC = SPF * SY
        most = max(sizes)
        vmem = pl.BlockSpec(memory_space=pltpu.VMEM)
        hbm = pl.BlockSpec(memory_space=pltpu.HBM)
        V = pltpu.VMEM
        D = pltpu.SemaphoreType.DMA
        return pl.pallas_call(
            functools.partial(kernel, sizes),
            out_shape=(jax.ShapeDtypeStruct(fine.shape, f32),
                       jax.ShapeDtypeStruct(coarse.shape, f32)),
            in_specs=[hbm] * 4,
            out_specs=(vmem, vmem),
            scratch_shapes=[
                V((SX, SY, SZ), f32), V((SX, SY, SZ), f32),
                V((3, PX, PY, PZ), f32), V(coarse.shape, f32),
                V((SX + 4, SY + 16, SZ), f32),
                V((2, SX, 2, SZ), f32), V((2, SX, 2, SZ), f32),
                V((2, SY, SZ), f32), V((2, SY, SZ), f32), V((2, SY, SZ), f32),
                V((2, 5 * QE, KC), bf16), V((SPC // SPF, 2, 4 * QC, KC), bf16),
                V((2, KC, 3 * SZ), bf16), V((2, KC, 3 * SZ), bf16),
                V((2, EX, PY, 3 * SZ), f32), V((KX + 4, QC, 3 * SZ), f32),
                V((2, 3, RZ, EX * PY), f32), V((2, 3, RZ, EX * PY), f32),
                V((3, KX * QC, KZ), f32), V((3, KX * QC, KZ), f32),
                V((2, 2, 8, EX * PY), f32), V((2, 2, 8, EX * PY), f32),
                V((2, 3 * PZ, EX * PY), f32), V((2, 3 * PZ, EX * PY), f32),
                V((3 * PZ, EX * PY), f32), V((2, 3 * PZ, EX * PY), f32),
                V((3, most, KZ, 3 * KX * QC), f32),
                D((2, SX // SPF)), D((2,)), D((3, 2)), D((3, 2)), D((2, 4)), D((2, 4)),
                D((3, 2)), D((3, 2)), D((3, most)), D((3, most)),
            ],
            compiler_params=pltpu.CompilerParams(
                collective_id=0, has_side_effects=True, vmem_limit_bytes=66000000
            ),
        )(warped, fixed, fine, coarse)

    in_specs = (P("gx", "gy", "gz"), P("gx", "gy", "gz"), P(None, "gx", "gy", "gz"), P())
    out_specs = (P(None, "gx", "gy", "gz"), P())
    return jax.shard_map(
        step, mesh=mesh, in_specs=in_specs, out_specs=out_specs, check_vma=False
    )
```
